32 devices in a mesh: row: 8 (over z, x), col: 4 (over y, core).
Axes of the slice: x: 2, y: 2, z: 4, core: 2. Of those that a mesh axis runs over, the one named last changes fastest.
Arguments:
- gradients: bfloat16 [32, 2, 524288], P(('row', 'col')), may hold values from -96 to 96
- master_params: float32 [2, 524288], P(None, ('row', 'col')), may hold values from -0.1 to 0.1
- first_moment: float32 [2, 524288], P(None, ('row', 'col')), may hold values from -3 to 3
- second_moment: float32 [2, 524288], P(None, ('row', 'col')), may hold values from 0.05 to 5
Outputs:
- new_master: float32 [2, 524288], P(None, ('row', 'col'))
- new_first: float32 [2, 524288], P(None, ('row', 'col'))
- new_second: float32 [2, 524288], P(None, ('row', 'col'))
- new_weights: bfloat16 [2, 524288], replicated
The draws below stay inside these ranges and needn't reach their ends.
All inputs are finite; a program needn't handle non-finite values.
Results may differ from the reference program's by a relative error of at most 0.009.
Values may be sent and summed in bfloat16 or wider, within the bound.
A program may use at most 64 MiB of HBM per device.

```python
import math
import jax
import jax.numpy as jnp
from jax import lax

LAYERS = 2
SLICE = 524288
DEVICES = 32


def spiked(result, rng, source, target, shards_of, factor):
    owner, partner = [(jnp.arange(result.shape[axis_at]) // (result.shape[axis_at] // shards_of)).reshape([-1 if axis == axis_at else 1 for axis in range(result.ndim)]) for axis_at in (source, target)]
    chosen = jax.random.permutation(rng, shards_of)[partner]
    strong = (owner == chosen) | (owner == (partner + shards_of // 2) % shards_of)
    return jnp.where(strong, factor * result, result)


def level_of(own_key, extent, split, smallest, largest):
    factor_of, own = 1.0, jax.random.fold_in(own_key, 6)
    for position, parts in split:
        heights = jnp.exp(jax.random.uniform(jax.random.fold_in(own, position), (parts,), jnp.float32, smallest / len(split), largest / len(split)))
        factor_of = factor_of * jnp.repeat(heights, extent[position] // parts).reshape([-1 if axis == position else 1 for axis in range(len(extent))])
    return factor_of


def gaussian(rng, dims, spread, most, split=(), held_as=jnp.bfloat16):
    result = jax.random.normal(rng, dims, jnp.float32) * spread
    if len(split) > 0:
        result = level_of(rng, dims, split, -0.22, 0.18) * result
    return jnp.clip(result, min=-most, max=most).astype(held_as)


def heavy_noise(own_key, dims, spread, bound, pieces, heavy, kind=jnp.bfloat16):
    drawn = spread * jax.random.normal(own_key, dims, jnp.float32)
    if pieces:
        drawn = drawn * level_of(own_key, dims, pieces, -0.22, 0.18)
    return jnp.clip(spiked(drawn, jax.random.fold_in(own_key, 3), *heavy), -bound, bound).astype(kind)


def setup_inputs(seed: int = 0) -> dict:
    splits = jax.random.split(jax.random.key(seed), 5)
    gradients = heavy_noise(splits[0], (DEVICES, LAYERS, SLICE), 16.0, 96.0, ((0, 32),), (0, 2, 32, 2.75))
    master_params = gaussian(splits[1], (LAYERS, SLICE), 0.025, 0.1, ((1, 32),), jnp.float32)
    first_moment = gaussian(splits[2], (LAYERS, SLICE), 0.5, 3.0, ((1, 32),), jnp.float32)
    second_moment = jnp.clip(jnp.exp(math.log(5.0) - 4.6051702 * jax.random.uniform(splits[3], (LAYERS, SLICE), jnp.float32) ** level_of(splits[3], (LAYERS, SLICE), ((1, 32),), -0.2, 0.2)), 0.05, 5.0)
    return {"gradients": gradients, "master_params": master_params, "first_moment": first_moment, "second_moment": second_moment}


beta_one = 0.9
beta_two = 0.95
learn_rate = 0.001
decay_rate = 0.1
epsilon = 1e-08
adam_step = 10.0

def adam_update(mean_grad, master_params, first_moment, second_moment):
    new_first = beta_one * first_moment + (1.0 - beta_one) * mean_grad
    new_second = beta_two * second_moment + (1.0 - beta_two) * mean_grad * mean_grad
    first_hat = new_first / (1.0 - beta_one ** adam_step)
    second_hat = new_second / (1.0 - beta_two ** adam_step)
    new_master = master_params - learn_rate * (first_hat / (jnp.sqrt(second_hat) + epsilon) + decay_rate * master_params)
    return (new_master, new_first, new_second)

def reference(gradients, master_params, first_moment, second_moment):
    mean_grad = lax.optimization_barrier(jnp.sum(gradients, axis=0, dtype=jnp.float32)) / DEVICES
    new_master, new_first, new_second = adam_update(mean_grad, master_params, first_moment, second_moment)
    return (new_master, new_first, new_second, new_master.astype(jnp.bfloat16))
```

```python
import functools

import jax
import jax.numpy as jnp
import numpy as np
from jax import lax
from jax.experimental import pallas as pl
from jax.experimental.pallas import tpu as pltpu
from jax.sharding import PartitionSpec as P

beta_one = 0.9
beta_two = 0.95
learn_rate = 0.001
decay_rate = 0.1
epsilon = 1e-08
adam_step = 10.0

LANES = 128
FLOWS = 4
MESH = pl.DeviceIdType.MESH


def adam_update(mean_grad, master_params, first_moment, second_moment):
    new_first = beta_one * first_moment + (1.0 - beta_one) * mean_grad
    new_second = beta_two * second_moment + (1.0 - beta_two) * mean_grad * mean_grad
    first_hat = new_first / (1.0 - beta_one**adam_step)
    second_hat = new_second / (1.0 - beta_two**adam_step)
    new_master = master_params - learn_rate * (
        first_hat / (jnp.sqrt(second_hat) + epsilon) + decay_rate * master_params
    )
    return (new_master, new_first, new_second)


def factors(n):
    out = []
    while n > 1:
        k = next(k for k in (4, 2, *range(3, n + 1)) if n % k == 0)
        out.append(k)
        n //= k
    return out


def digits_of(rows, cols):
    core = [2] if cols % 2 == 0 else []
    found = []
    for axis, sizes in (("row", factors(rows)), ("col", factors(cols // (2 if core else 1)) + core)):
        stride = int(np.prod(sizes, dtype=np.int64))
        for size in sizes:
            stride //= size
            found.append((axis, size, stride))
    return found


def orders_of(digits):
    last = len(digits) - 1
    row_at = [i for i in range(last) if digits[i][0] == "row"]
    col_at = [i for i in range(last) if digits[i][0] == "col"]
    x, y = row_at[-1:], col_at[:1]
    rest = col_at[1:] + row_at[:-1]
    return ([last] + x + y + rest, [last] + y + x + rest)


def kernel(digits, flow_orders, r, grad, master, first, second, new_master, new_first, new_second, weights, scratch):
    count = len(digits)
    devices = int(np.prod([d[1] for d in digits]))
    at = {axis: lax.axis_index(axis) for axis in ("row", "col")}
    mine = [lax.rem(at[axis] // stride, size) for axis, size, stride in digits]

    def peer(digit, t):
        axis, size, stride = digits[digit]
        value = lax.rem(mine[digit] + t, size)
        ids = dict(at)
        ids[axis] = at[axis] + (value - mine[digit]) * stride
        return value, (ids["row"], ids["col"])

    flows = len(flow_orders)
    rows = [pl.ds(f * r, r) for f in range(flows)]

    loads = []
    for f in range(flows):
        digit = flow_orders[f][0]
        where = tuple(mine[i] if i == digit else slice(None) for i in range(count)) + (rows[f],)
        copy = pltpu.make_async_copy(grad.at[where], scratch["own"].at[f], scratch["load_sem"].at[f])
        copy.start()
        loads.append(copy)
    states = []
    for i, (src, name) in enumerate(((master, "master"), (first, "first"), (second, "second"))):
        copy = pltpu.make_async_copy(src, scratch[name], scratch["load_sem"].at[flows + i])
        copy.start()
        states.append(copy)

    barrier = pltpu.get_barrier_semaphore()
    greeted = 0
    for digit in range(count):
        for t in range(1, digits[digit][1]):
            pl.semaphore_signal(barrier, inc=1, device_id=peer(digit, t)[1], device_id_type=MESH)
            greeted += 1
    pl.semaphore_wait(barrier, greeted)

    sent = []
    pending = {}

    def send(f, step, digit, t, src, dst, device):
        copy = pltpu.make_async_remote_copy(
            src_ref=src,
            dst_ref=dst,
            send_sem=scratch["send_sem"].at[f, step, t - 1],
            recv_sem=scratch["recv_sem"].at[f, step, t - 1],
            device_id=device,
            device_id_type=MESH,
        )
        copy.start()
        sent.append(copy)
        pending.setdefault((f, step), []).append(copy)

    def scatter(f, p):
        digit = flow_orders[f][p]
        left = sorted(flow_orders[f][p:])
        for t in range(1, digits[digit][1]):
            value, device = peer(digit, t)
            where = tuple(value if i == digit else slice(None) for i in left)
            src = grad.at[where + (rows[f],)] if p == 0 else scratch[f"sum{f}_{p}"].at[where]
            send(f, p, digit, t, src, scratch[f"got{f}_{p}"].at[t - 1], device)

    def gather(f, p):
        digit = flow_orders[f][p]
        have = set(flow_orders[f][p + 1 :])
        where = tuple(slice(None) if i in have else mine[i] for i in range(count)) + (rows[f],)
        for t in range(1, digits[digit][1]):
            send(f, 2 * count - 1 - p, digit, t, weights.at[where], weights.at[where], peer(digit, t)[1])

    def arrived(f, step):
        for copy in pending[(f, step)]:
            copy.wait_recv()

    for f in range(flows):
        scatter(f, 0)
    for p in range(count):
        for f in range(flows):
            digit = flow_orders[f][p]
            left = sorted(flow_orders[f][p:])
            after = sorted(flow_orders[f][p + 1 :])
            if p == 0:
                loads[f].wait()
            arrived(f, p)
            got = scratch[f"got{f}_{p}"]
            last = p == count - 1
            for idx in np.ndindex(*(digits[i][1] for i in after)):
                if p == 0:
                    total = scratch["own"][(f,) + idx].astype(jnp.float32)
                else:
                    place = dict(zip(after, idx))
                    total = scratch[f"sum{f}_{p}"][
                        tuple(mine[digit] if i == digit else place[i] for i in left)
                    ].astype(jnp.float32)
                for t in range(digits[digit][1] - 1):
                    total += got[(t,) + idx].astype(jnp.float32)
                if not last:
                    scratch[f"sum{f}_{p + 1}"][idx] = total.astype(jnp.bfloat16)
            if not last:
                scatter(f, p + 1)
                continue
            if f == 0:
                for copy in states:
                    copy.wait()
            updated, moment, variance = adam_update(
                total / devices, scratch["master"][rows[f], :], scratch["first"][rows[f], :], scratch["second"][rows[f], :]
            )
            weights[tuple(mine) + (rows[f],)] = updated.astype(jnp.bfloat16)
            gather(f, count - 1)
            new_master[rows[f], :] = updated
            new_first[rows[f], :] = moment
            new_second[rows[f], :] = variance
    for p in reversed(range(count)):
        for f in range(flows):
            arrived(f, 2 * count - 1 - p)
            if p > 0:
                gather(f, p - 1)
    for copy in sent:
        copy.wait_send()


def to_rows(x):
    layers, length = x.shape
    return x.reshape(layers, length // LANES, LANES).transpose(1, 0, 2).reshape(layers * length // LANES, LANES)


def from_rows(x, layers):
    total = x.shape[0]
    return x.reshape(total // layers, layers, LANES).transpose(1, 0, 2).reshape(layers, total // layers * LANES)


def shards(digits, gradients, master_params, first_moment, second_moment):
    count = len(digits)
    sizes = tuple(d[1] for d in digits)
    devices = int(np.prod(sizes))
    layers = gradients.shape[1]
    grad = to_rows(gradients[0])
    block = grad.shape[0] // devices
    flows = next(n for n in (FLOWS, 2, 1) if block % n == 0 and (block // n) % 16 == 0)
    r = block // flows
    orders = orders_of(digits)
    flow_orders = [orders[f % len(orders)] for f in range(flows)]

    most = max(sizes) - 1
    scratch = {
        "own": pltpu.VMEM((flows,) + sizes[:-1] + (r, LANES), jnp.bfloat16),
        "load_sem": pltpu.SemaphoreType.DMA((flows + 3,)),
        "send_sem": pltpu.SemaphoreType.DMA((flows, 2 * count, most)),
        "recv_sem": pltpu.SemaphoreType.DMA((flows, 2 * count, most)),
    }
    for name in ("master", "first", "second"):
        scratch[name] = pltpu.VMEM((block, LANES), jnp.float32)
    for f, order in enumerate(flow_orders):
        for p in range(count):
            left = tuple(sizes[i] for i in sorted(order[p:]))
            after = tuple(sizes[i] for i in sorted(order[p + 1 :]))
            if p > 0:
                scratch[f"sum{f}_{p}"] = pltpu.VMEM(left + (r, LANES), jnp.bfloat16)
            scratch[f"got{f}_{p}"] = pltpu.VMEM((sizes[order[p]] - 1,) + after + (r, LANES), jnp.bfloat16)

    any_spec = pl.BlockSpec(memory_space=pl.ANY)
    vmem_spec = pl.BlockSpec(memory_space=pltpu.VMEM)
    part = jax.ShapeDtypeStruct((block, LANES), jnp.float32)
    names = list(scratch)

    def body(*refs):
        kernel(digits, flow_orders, r, *refs[:8], dict(zip(names, refs[8:])))

    new_master, new_first, new_second, weights = pl.pallas_call(
        body,
        name="average_update",
        out_shape=(part, part, part, jax.ShapeDtypeStruct(sizes + (block, LANES), jnp.bfloat16)),
        in_specs=[any_spec] * 4,
        out_specs=(vmem_spec,) * 4,
        scratch_shapes=[scratch[name] for name in names],
        compiler_params=pltpu.CompilerParams(
            collective_id=0, has_side_effects=True, vmem_limit_bytes=40 * 1024 * 1024
        ),
    )(grad.reshape(sizes + (block, LANES)), to_rows(master_params), to_rows(first_moment), to_rows(second_moment))
    return (
        from_rows(new_master, layers),
        from_rows(new_first, layers),
        from_rows(new_second, layers),
        from_rows(weights.reshape(devices * block, LANES), layers),
    )


def solution(mesh):
    digits = digits_of(mesh.shape["row"], mesh.shape["col"])
    in_specs = (
        P(("row", "col"), None, None),
        P(None, ("row", "col")),
        P(None, ("row", "col")),
        P(None, ("row", "col")),
    )
    out_specs = (P(None, ("row", "col")), P(None, ("row", "col")), P(None, ("row", "col")), P())
    return jax.shard_map(
        functools.partial(shards, digits), mesh=mesh, in_specs=in_specs, out_specs=out_specs, check_vma=False
    )
```

```python
import functools

import jax
import jax.numpy as jnp
import numpy as np
from jax import lax
from jax.experimental import pallas as pl
from jax.experimental.pallas import tpu as pltpu
from jax.sharding import PartitionSpec as P

beta_one = 0.9
beta_two = 0.95
learn_rate = 0.001
decay_rate = 0.1
epsilon = 1e-08
adam_step = 10.0

LANES = 128
FLOWS = 4
VMEM_LIMIT = 40 * 1024 * 1024
MESH = pl.DeviceIdType.MESH


def adam_update(mean_grad, master_params, first_moment, second_moment):
    new_first = beta_one * first_moment + (1.0 - beta_one) * mean_grad
    new_second = beta_two * second_moment + (1.0 - beta_two) * mean_grad * mean_grad
    first_hat = new_first / (1.0 - beta_one**adam_step)
    second_hat = new_second / (1.0 - beta_two**adam_step)
    new_master = master_params - learn_rate * (
        first_hat / (jnp.sqrt(second_hat) + epsilon) + decay_rate * master_params
    )
    return (new_master, new_first, new_second)


def factors(n):
    out = []
    while n > 1:
        k = next(k for k in (4, 2, *range(3, n + 1)) if n % k == 0)
        out.append(k)
        n //= k
    return out


def digits_of(rows, cols):
    core = [2] if cols % 2 == 0 else []
    found = []
    for axis, sizes in (("row", factors(rows)), ("col", factors(cols // (2 if core else 1)) + core)):
        stride = int(np.prod(sizes, dtype=np.int64))
        for size in sizes:
            stride //= size
            found.append((axis, size, stride))
    return found


def orders_of(digits):
    last = len(digits) - 1
    row_at = [i for i in range(last) if digits[i][0] == "row"]
    col_at = [i for i in range(last) if digits[i][0] == "col"]
    x, y = row_at[-1:], col_at[:1]
    rest = col_at[1:] + row_at[:-1]
    return ([last] + x + y + rest, [last] + y + x + rest)


def kernel(digits, flow_orders, r, grad, master, first, second, new_master, new_first, new_second, weights, scratch):
    count = len(digits)
    devices = int(np.prod([d[1] for d in digits]))
    at = {axis: lax.axis_index(axis) for axis in ("row", "col")}
    mine = [lax.rem(at[axis] // stride, size) for axis, size, stride in digits]

    def peer(digit, t):
        axis, size, stride = digits[digit]
        value = lax.rem(mine[digit] + t, size)
        ids = dict(at)
        ids[axis] = at[axis] + (value - mine[digit]) * stride
        return value, (ids["row"], ids["col"])

    flows = len(flow_orders)
    rows = [pl.ds(f * r, r) for f in range(flows)]

    loads = {}
    for keep in (0, 1):
        for f in range(flows):
            digit = flow_orders[f][0]
            for t in [0] if keep else range(1, digits[digit][1]):
                value = peer(digit, t)[0]
                where = tuple(value if i == digit else slice(None) for i in range(count)) + (rows[f],)
                loads[f, t] = pltpu.make_async_copy(
                    grad.at[where], scratch[f"raw{f}"].at[t], scratch["load_sem"].at[f, t]
                )
                loads[f, t].start()
    states = []
    for i, (src, name) in enumerate(((master, "master"), (first, "first"), (second, "second"))):
        copy = pltpu.make_async_copy(src, scratch[name], scratch["state_sem"].at[i])
        copy.start()
        states.append(copy)

    barrier = pltpu.get_barrier_semaphore()
    greeted = 0
    for digit in range(count):
        for t in range(1, digits[digit][1]):
            pl.semaphore_signal(barrier, inc=1, device_id=peer(digit, t)[1], device_id_type=MESH)
            greeted += 1
    pl.semaphore_wait(barrier, greeted)

    sent = []
    pending = {}

    def send(f, step, digit, t, src, dst, device):
        copy = pltpu.make_async_remote_copy(
            src_ref=src,
            dst_ref=dst,
            send_sem=scratch["send_sem"].at[f, step, t - 1],
            recv_sem=scratch["recv_sem"].at[f, step, t - 1],
            device_id=device,
            device_id_type=MESH,
        )
        copy.start()
        sent.append(copy)
        pending.setdefault((f, step), []).append(copy)

    def total(f, p, place):
        order = flow_orders[f]
        value = scratch[f"raw{f}"][(0,) + tuple(place.get(i, mine[i]) for i in sorted(order[1:]))].astype(jnp.float32)
        for q in range(p):
            after = tuple(place.get(i, mine[i]) for i in sorted(order[q + 1 :]))
            for t in range(digits[order[q]][1] - 1):
                value += scratch[f"got{f}_{q}"][(t,) + after].astype(jnp.float32)
        return value

    def scatter(f, p):
        digit = flow_orders[f][p]
        after = sorted(flow_orders[f][p + 1 :])
        for t in range(1, digits[digit][1]):
            value, device = peer(digit, t)
            if p == 0:
                loads[f, t].wait()
                src = scratch[f"raw{f}"].at[t]
            else:
                src = scratch[f"sum{f}_{p}"].at[t - 1]
                for idx in np.ndindex(*(digits[i][1] for i in after)):
                    place = dict(zip(after, idx))
                    place[digit] = value
                    src[idx] = total(f, p, place).astype(jnp.bfloat16)
            send(f, p, digit, t, src, scratch[f"got{f}_{p}"].at[t - 1], device)

    def gather(f, p):
        digit = flow_orders[f][p]
        have = set(flow_orders[f][p + 1 :])
        where = tuple(slice(None) if i in have else mine[i] for i in range(count)) + (rows[f],)
        for t in range(1, digits[digit][1]):
            send(f, 2 * count - 1 - p, digit, t, weights.at[where], weights.at[where], peer(digit, t)[1])

    def arrived(f, step):
        for copy in pending[(f, step)]:
            copy.wait_recv()

    for f in range(flows):
        scatter(f, 0)
    for p in range(count):
        for f in range(flows):
            if p == 0:
                loads[f, 0].wait()
            arrived(f, p)
            if p < count - 1:
                scatter(f, p + 1)
                continue
            if f == 0:
                for copy in states:
                    copy.wait()
            updated, moment, variance = adam_update(
                total(f, count, {}) / devices,
                scratch["master"][rows[f], :],
                scratch["first"][rows[f], :],
                scratch["second"][rows[f], :],
            )
            weights[tuple(mine) + (rows[f],)] = updated.astype(jnp.bfloat16)
            gather(f, count - 1)
            new_master[rows[f], :] = updated
            new_first[rows[f], :] = moment
            new_second[rows[f], :] = variance
    for p in reversed(range(count)):
        for f in range(flows):
            arrived(f, 2 * count - 1 - p)
            if p > 0:
                gather(f, p - 1)
    for copy in sent:
        copy.wait_send()


def to_rows(x):
    layers, length = x.shape
    return x.reshape(layers, length // LANES, LANES).transpose(1, 0, 2).reshape(layers * length // LANES, LANES)


def from_rows(x, layers):
    total = x.shape[0]
    return x.reshape(total // layers, layers, LANES).transpose(1, 0, 2).reshape(layers, total // layers * LANES)


def write_out(*arrays):
    count = len(arrays)

    def body(*refs):
        copies = [pltpu.make_async_copy(refs[i], refs[count + i], refs[-1].at[i]) for i in range(count)]
        for copy in copies[::-1]:
            copy.start()
        for copy in copies:
            copy.wait()

    return pl.pallas_call(
        body,
        name="write_out",
        out_shape=tuple(jax.ShapeDtypeStruct(x.shape, x.dtype) for x in arrays),
        in_specs=[pl.BlockSpec(memory_space=pltpu.VMEM)] * count,
        out_specs=(pl.BlockSpec(memory_space=pltpu.HBM),) * count,
        scratch_shapes=[pltpu.SemaphoreType.DMA((count,))],
        compiler_params=pltpu.CompilerParams(vmem_limit_bytes=1 << 20),
    )(*arrays)


def shards(digits, gradients, master_params, first_moment, second_moment):
    count = len(digits)
    sizes = tuple(d[1] for d in digits)
    devices = int(np.prod(sizes))
    layers = gradients.shape[1]
    grad = to_rows(gradients[0])
    block = grad.shape[0] // devices
    flows = next(n for n in (FLOWS, 2, 1) if block % n == 0 and (block // n) % 16 == 0)
    r = block // flows
    orders = orders_of(digits)
    flow_orders = [orders[f % len(orders)] for f in range(flows)]

    most = max(sizes) - 1
    scratch = {
        "load_sem": pltpu.SemaphoreType.DMA((flows, most + 1)),
        "state_sem": pltpu.SemaphoreType.DMA((3,)),
        "send_sem": pltpu.SemaphoreType.DMA((flows, 2 * count, most)),
        "recv_sem": pltpu.SemaphoreType.DMA((flows, 2 * count, most)),
    }
    for name in ("master", "first", "second"):
        scratch[name] = pltpu.VMEM((block, LANES), jnp.float32)
    for f, order in enumerate(flow_orders):
        for p in range(count):
            after = tuple(sizes[i] for i in sorted(order[p + 1 :])) + (r, LANES)
            if p == 0:
                scratch[f"raw{f}"] = pltpu.VMEM((sizes[order[p]],) + after, jnp.bfloat16)
            else:
                scratch[f"sum{f}_{p}"] = pltpu.VMEM((sizes[order[p]] - 1,) + after, jnp.bfloat16)
            scratch[f"got{f}_{p}"] = pltpu.VMEM((sizes[order[p]] - 1,) + after, jnp.bfloat16)

    hbm_spec = pl.BlockSpec(memory_space=pltpu.HBM)
    vmem_spec = pl.BlockSpec(memory_space=pltpu.VMEM)
    part = jax.ShapeDtypeStruct((block, LANES), jnp.float32)
    names = list(scratch)

    def body(*refs):
        kernel(digits, flow_orders, r, *refs[:8], dict(zip(names, refs[8:])))

    new_master, new_first, new_second, weights = pl.pallas_call(
        body,
        name="average_update",
        out_shape=(part, part, part, jax.ShapeDtypeStruct(sizes + (block, LANES), jnp.bfloat16)),
        in_specs=[hbm_spec] * 4,
        out_specs=(vmem_spec,) * 4,
        scratch_shapes=[scratch[name] for name in names],
        compiler_params=pltpu.CompilerParams(
            collective_id=0, has_side_effects=True, vmem_limit_bytes=VMEM_LIMIT
        ),
    )(
        *(
            pltpu.with_memory_space_constraint(x, pltpu.HBM)
            for x in (
                grad.reshape(sizes + (block, LANES)),
                to_rows(master_params),
                to_rows(first_moment),
                to_rows(second_moment),
            )
        )
    )
    results = write_out(new_master, new_first, new_second, weights.reshape(devices * block, LANES))
    return tuple(from_rows(x, layers) for x in results)


def solution(mesh):
    digits = digits_of(mesh.shape["row"], mesh.shape["col"])
    in_specs = (
        P(("row", "col"), None, None),
        P(None, ("row", "col")),
        P(None, ("row", "col")),
        P(None, ("row", "col")),
    )
    out_specs = (P(None, ("row", "col")), P(None, ("row", "col")), P(None, ("row", "col")), P())
    return jax.shard_map(
        functools.partial(shards, digits), mesh=mesh, in_specs=in_specs, out_specs=out_specs, check_vma=False
    )
```

```python
import functools

import jax
import jax.numpy as jnp
import numpy as np
from jax import lax
from jax.experimental import pallas as pl
from jax.experimental.pallas import tpu as pltpu
from jax.sharding import PartitionSpec as P

beta_one = 0.9
beta_two = 0.95
learn_rate = 0.001
decay_rate = 0.1
epsilon = 1e-08
adam_step = 10.0

LANES = 128
SPLIT = ((56, "x"), (56, "y"), (48, "x"), (48, "y"), (48, "z"))
STEP_ROWS = 8
VMEM_LIMIT = 40 * 1024 * 1024
MESH = pl.DeviceIdType.MESH


def adam_update(mean_grad, master_params, first_moment, second_moment):
    new_first = beta_one * first_moment + (1.0 - beta_one) * mean_grad
    new_second = beta_two * second_moment + (1.0 - beta_two) * mean_grad * mean_grad
    first_hat = new_first / (1.0 - beta_one**adam_step)
    second_hat = new_second / (1.0 - beta_two**adam_step)
    new_master = master_params - learn_rate * (
        first_hat / (jnp.sqrt(second_hat) + epsilon) + decay_rate * master_params
    )
    return (new_master, new_first, new_second)


def factors(n):
    out = []
    while n > 1:
        k = next(k for k in (4, 2, *range(3, n + 1)) if n % k == 0)
        out.append(k)
        n //= k
    return out


def digits_of(rows, cols):
    core = [2] if cols % 2 == 0 else []
    found = []
    for axis, sizes in (("row", factors(rows)), ("col", factors(cols // (2 if core else 1)) + core)):
        stride = int(np.prod(sizes, dtype=np.int64))
        for size in sizes:
            stride //= size
            found.append((axis, size, stride))
    return found


def orders_of(digits):
    last = len(digits) - 1
    row_at = [i for i in range(last) if digits[i][0] == "row"]
    col_at = [i for i in range(last) if digits[i][0] == "col"]
    x, y = row_at[-1:], col_at[:1]
    rest = col_at[1:] + row_at[:-1]
    return {"x": [last] + x + y + rest, "y": [last] + y + x + rest, "z": [last] + rest + x + y, "w": [last] + rest + y + x}


def kernel(digits, flow_orders, rows, grad, master, first, second, new_master, new_first, new_second, weights, scratch):
    count = len(digits)
    devices = int(np.prod([d[1] for d in digits]))
    at = {axis: lax.axis_index(axis) for axis in ("row", "col")}
    mine = [lax.rem(at[axis] // stride, size) for axis, size, stride in digits]

    def peer(digit, t):
        axis, size, stride = digits[digit]
        value = lax.rem(mine[digit] + t, size)
        ids = dict(at)
        ids[axis] = at[axis] + (value - mine[digit]) * stride
        return value, (ids["row"], ids["col"])

    flows = len(flow_orders)

    loads = {}
    for keep in (0, 1):
        for f in range(flows):
            digit = flow_orders[f][0]
            for t in [0] if keep else range(1, digits[digit][1]):
                value = peer(digit, t)[0]
                where = tuple(value if i == digit else slice(None) for i in range(count)) + (rows[f],)
                loads[f, t] = pltpu.make_async_copy(
                    grad.at[where], scratch[f"raw{f}"].at[t], scratch["load_sem"].at[f, t]
                )
                loads[f, t].start()
    states = []
    for i, (src, name) in enumerate(((master, "master"), (first, "first"), (second, "second"))):
        copy = pltpu.make_async_copy(src, scratch[name], scratch["state_sem"].at[i])
        copy.start()
        states.append(copy)

    barrier = pltpu.get_barrier_semaphore()
    greeted = 0
    for digit in range(count):
        for t in range(1, digits[digit][1]):
            pl.semaphore_signal(barrier, inc=1, device_id=peer(digit, t)[1], device_id_type=MESH)
            greeted += 1
    pl.semaphore_wait(barrier, greeted)

    sent = []
    pending = {}

    def send(f, step, digit, t, src, dst, device):
        copy = pltpu.make_async_remote_copy(
            src_ref=src,
            dst_ref=dst,
            send_sem=scratch["send_sem"].at[f, step, t - 1],
            recv_sem=scratch["recv_sem"].at[f, step, t - 1],
            device_id=device,
            device_id_type=MESH,
        )
        copy.start()
        sent.append(copy)
        pending.setdefault((f, step), []).append(copy)

    def total(f, p, place):
        order = flow_orders[f]
        value = scratch[f"raw{f}"][(0,) + tuple(place.get(i, mine[i]) for i in sorted(order[1:]))].astype(jnp.float32)
        for q in range(p):
            after = tuple(place.get(i, mine[i]) for i in sorted(order[q + 1 :]))
            for t in range(digits[order[q]][1] - 1):
                value += scratch[f"got{f}_{q}"][(t,) + after].astype(jnp.float32)
        return value

    def scatter(f, p):
        digit = flow_orders[f][p]
        after = sorted(flow_orders[f][p + 1 :])
        for t in range(1, digits[digit][1]):
            value, device = peer(digit, t)
            if p == 0:
                loads[f, t].wait()
                src = scratch[f"raw{f}"].at[t]
            else:
                src = scratch[f"sum{f}_{p}"].at[t - 1]
                for idx in np.ndindex(*(digits[i][1] for i in after)):
                    place = dict(zip(after, idx))
                    place[digit] = value
                    src[idx] = total(f, p, place).astype(jnp.bfloat16)
            send(f, p, digit, t, src, scratch[f"got{f}_{p}"].at[t - 1], device)

    def gather(f, p):
        digit = flow_orders[f][p]
        have = set(flow_orders[f][p + 1 :])
        where = tuple(slice(None) if i in have else mine[i] for i in range(count)) + (rows[f],)
        for t in range(1, digits[digit][1]):
            send(f, 2 * count - 1 - p, digit, t, weights.at[where], weights.at[where], peer(digit, t)[1])

    def arrived(f, step):
        for copy in pending[(f, step)]:
            copy.wait_recv()

    for f in range(flows):
        scatter(f, 0)
    def update(f):
        if f == 0:
            for copy in states:
                copy.wait()
        updated, moment, variance = adam_update(
            total(f, count, {}) / devices,
            scratch["master"][rows[f], :],
            scratch["first"][rows[f], :],
            scratch["second"][rows[f], :],
        )
        weights[tuple(mine) + (rows[f],)] = updated.astype(jnp.bfloat16)
        gather(f, count - 1)
        new_master[rows[f], :] = updated
        new_first[rows[f], :] = moment
        new_second[rows[f], :] = variance

    turns = [(step, f) for step in range(2 * count) for f in range(flows)]
    for step, f in turns:
        if step == 0:
            loads[f, 0].wait()
        arrived(f, step)
        if step < count - 1:
            scatter(f, step + 1)
        elif step == count - 1:
            update(f)
        elif step < 2 * count - 1:
            gather(f, 2 * count - 2 - step)
    for copy in sent:
        copy.wait_send()


def to_rows(x):
    layers, length = x.shape
    return x.reshape(layers, length // LANES, LANES).transpose(1, 0, 2).reshape(layers * length // LANES, LANES)


def from_rows(x, layers):
    total = x.shape[0]
    return x.reshape(total // layers, layers, LANES).transpose(1, 0, 2).reshape(layers, total // layers * LANES)


def write_out(*arrays):
    count = len(arrays)

    def body(*refs):
        copies = [pltpu.make_async_copy(refs[i], refs[count + i], refs[-1].at[i]) for i in range(count)]
        for copy in copies[::-1]:
            copy.start()
        for copy in copies:
            copy.wait()

    return pl.pallas_call(
        body,
        name="write_out",
        out_shape=tuple(jax.ShapeDtypeStruct(x.shape, x.dtype) for x in arrays),
        in_specs=[pl.BlockSpec(memory_space=pltpu.VMEM)] * count,
        out_specs=(pl.BlockSpec(memory_space=pltpu.HBM),) * count,
        scratch_shapes=[pltpu.SemaphoreType.DMA((count,))],
        compiler_params=pltpu.CompilerParams(vmem_limit_bytes=1 << 20),
    )(*arrays)


def shards(digits, gradients, master_params, first_moment, second_moment):
    count = len(digits)
    sizes = tuple(d[1] for d in digits)
    devices = int(np.prod(sizes))
    layers = gradients.shape[1]
    grad = to_rows(gradients[0])
    block = grad.shape[0] // devices
    orders = orders_of(digits)
    whole, start, done = sum(share for share, _ in SPLIT), 0, 0
    flow_orders, rows = [], []
    for share, name in SPLIT:
        done += share
        end = block if done == whole else done * block // whole // STEP_ROWS * STEP_ROWS
        if end > start:
            flow_orders.append(orders[name])
            rows.append(pl.ds(start, end - start))
            start = end
    flows = len(rows)

    most = max(sizes) - 1
    scratch = {
        "load_sem": pltpu.SemaphoreType.DMA((flows, most + 1)),
        "state_sem": pltpu.SemaphoreType.DMA((3,)),
        "send_sem": pltpu.SemaphoreType.DMA((flows, 2 * count, most)),
        "recv_sem": pltpu.SemaphoreType.DMA((flows, 2 * count, most)),
    }
    for name in ("master", "first", "second"):
        scratch[name] = pltpu.VMEM((block, LANES), jnp.float32)
    for f, order in enumerate(flow_orders):
        for p in range(count):
            after = tuple(sizes[i] for i in sorted(order[p + 1 :])) + (rows[f].size, LANES)
            if p == 0:
                scratch[f"raw{f}"] = pltpu.VMEM((sizes[order[p]],) + after, jnp.bfloat16)
            else:
                scratch[f"sum{f}_{p}"] = pltpu.VMEM((sizes[order[p]] - 1,) + after, jnp.bfloat16)
            scratch[f"got{f}_{p}"] = pltpu.VMEM((sizes[order[p]] - 1,) + after, jnp.bfloat16)

    hbm_spec = pl.BlockSpec(memory_space=pltpu.HBM)
    vmem_spec = pl.BlockSpec(memory_space=pltpu.VMEM)
    part = jax.ShapeDtypeStruct((block, LANES), jnp.float32)
    names = list(scratch)

    def body(*refs):
        kernel(digits, flow_orders, rows, *refs[:8], dict(zip(names, refs[8:])))

    new_master, new_first, new_second, weights = pl.pallas_call(
        body,
        name="average_update",
        out_shape=(part, part, part, jax.ShapeDtypeStruct(sizes + (block, LANES), jnp.bfloat16)),
        in_specs=[hbm_spec] * 4,
        out_specs=(vmem_spec,) * 4,
        scratch_shapes=[scratch[name] for name in names],
        compiler_params=pltpu.CompilerParams(
            collective_id=0, has_side_effects=True, vmem_limit_bytes=VMEM_LIMIT
        ),
    )(
        *(
            pltpu.with_memory_space_constraint(x, pltpu.HBM)
            for x in (
                grad.reshape(sizes + (block, LANES)),
                to_rows(master_params),
                to_rows(first_moment),
                to_rows(second_moment),
            )
        )
    )
    results = write_out(new_master, new_first, new_second, weights.reshape(devices * block, LANES))
    return tuple(from_rows(x, layers) for x in results)


def solution(mesh):
    digits = digits_of(mesh.shape["row"], mesh.shape["col"])
    in_specs = (
        P(("row", "col"), None, None),
        P(None, ("row", "col")),
        P(None, ("row", "col")),
        P(None, ("row", "col")),
    )
    out_specs = (P(None, ("row", "col")), P(None, ("row", "col")), P(None, ("row", "col")), P())
    return jax.shard_map(
        functools.partial(shards, digits), mesh=mesh, in_specs=in_specs, out_specs=out_specs, check_vma=False
    )
```
